32 devices in a mesh: gx: 4 (over x, core), gy: 2 (over y), gz: 4 (over z).
Axes of the slice: x: 2, y: 2, z: 4, core: 2. Of those that a mesh axis runs over, the one named last changes fastest.
Arguments:
- offsets: float32 [3, 4, 4, 8, 128], P(None, 'gx', 'gy', 'gz'), may hold values from 0 to 11, as said below
- type_ids: int32 [4, 4, 8, 128], P('gx', 'gy', 'gz'), may hold values from 0 to 1
- neighbours: int32 [4, 4, 8, 27], P('gx', 'gy', 'gz'), may hold values from 0 to 48, as said below
- type_chi: float32 [2], replicated, may hold values from 3 to 7
- type_eta: float32 [2], replicated, may hold values from 6 to 12
- type_gamma: float32 [2], replicated, may hold values from 0.5 to 1
Outputs:
- charges: float32 [4, 4, 8, 128], P('gx', 'gy', 'gz')
- residuals: float32 [2, 4, 4, 8, 128], P(None, 'gx', 'gy', 'gz')
The draws below stay inside these ranges and needn't reach their ends.
Inputs may be any that keep to these rules, and one draw needn't show every extreme that they name: `neighbours`: each tile's row lists the tile itself and some of the 26 cells around it, each at most once, as indices into its device's block padded by one cell on every side (3) x (4) x (4) in first-dimension-major order; unused slots hold (3) * 4 * 4. Two tiles list each other with opposite displacements or not at all. `offsets`: any two atoms of the box lie at least 0.8 A apart.
All inputs are finite; a program needn't handle non-finite values.
Results may differ from the reference program's by a relative error of at most 0.0003.
Values sent between devices are 32-bit elements; how exact they have to be, the bound alone decides.
A program may use at most 64 MiB of HBM per device.

```python
import jax
import jax.numpy as jnp
import numpy as np
from jax import lax

ATOMS = 128
NB = 27
TYPES = 2
ITERS = 3
CX = 1
CY = 2
CZ = 2
NCX = 4
NCY = 4
NCZ = 8


def lattice_sites():
    side = 1
    while (side + 1) ** 3 <= ATOMS:
        side = side + 1
    spacing = 11.0 / side
    points = []
    for first_step in range(side):
        for second_step in range(side):
            for third_step in range(side):
                points.append([(first_step + 0.5) * spacing, (second_step + 0.5) * spacing, (third_step + 0.5) * spacing])
    inner = max(side - 1, 1)
    extra_count = ATOMS - side ** 3
    for extra_index in range(extra_count):
        first_step = extra_index // (inner * inner)
        second_step = extra_index // inner % inner
        third_step = extra_index % inner
        points.append([spacing, spacing, (third_step + 1.0) * spacing])
    return np.array(points, dtype=np.float32).T


def draw_offsets(key, part):
    base = jnp.asarray(lattice_sites())[:, None, None, None, :]
    jitter = jnp.clip(0.12 * jax.random.normal(key, (3, NCX, NCY, NCZ, ATOMS), jnp.float32), -0.3, 0.3)
    return jnp.clip(base + jitter, 0.0, 10.999).astype(jnp.float32)


def draw_neighbours(key, part):
    offset_table = np.array([[first_step, second_step, third_step] for first_step in (-1, 0, 1) for second_step in (-1, 0, 1) for third_step in (-1, 0, 1)], dtype=np.int32)
    keep_bits = jax.random.randint(key, (NCX, NCY, NCZ, 13), 0, 4) > 0
    columns = []
    for slot_index in range(27):
        if slot_index < 13:
            columns.append(keep_bits[..., slot_index])
        elif slot_index == 13:
            columns.append(jnp.ones((NCX, NCY, NCZ), dtype=bool))
        else:
            mirror = 26 - slot_index
            moved = offset_table[slot_index]
            columns.append(jnp.roll(keep_bits[..., mirror], shift=(-int(moved[0]), -int(moved[1]), -int(moved[2])), axis=(0, 1, 2)))
    kept = jnp.stack(columns, -1)
    local_one = (jnp.arange(NCX, dtype=jnp.int32) % CX)[:, None, None, None]
    local_two = (jnp.arange(NCY, dtype=jnp.int32) % CY)[None, :, None, None]
    local_three = (jnp.arange(NCZ, dtype=jnp.int32) % CZ)[None, None, :, None]
    table_one = jnp.asarray(offset_table[:, 0])[None, None, None, :]
    table_two = jnp.asarray(offset_table[:, 1])[None, None, None, :]
    table_three = jnp.asarray(offset_table[:, 2])[None, None, None, :]
    padded_index = ((local_one + 1 + table_one) * (CY + 2) + (local_two + 1 + table_two)) * (CZ + 2) + (local_three + 1 + table_three)
    padded_index = jnp.broadcast_to(padded_index, (NCX, NCY, NCZ, 27))
    sentinel = (CX + 2) * (CY + 2) * (CZ + 2)
    slot_order = jnp.arange(27, dtype=jnp.int32)[None, None, None, :]
    order_key = jnp.where(kept, slot_order, slot_order + 27)
    order = jnp.argsort(order_key, axis=-1, stable=True)
    index_sorted = jnp.take_along_axis(padded_index, order, -1)
    kept_sorted = jnp.take_along_axis(kept, order, -1)
    return jnp.where(kept_sorted, index_sorted, sentinel).astype(jnp.int32)


def touch_ends(values, stream_key, least, top_value):
    shape = values.shape
    spot = [jax.random.randint(jax.random.fold_in(stream_key, axis), (), 0, shape[axis]) for axis in range(len(shape))]
    values = values.at[tuple(spot)].set(least)
    longest = shape.index(max(shape))
    spot[longest] = (spot[longest] + 1) % shape[longest]
    return values.at[tuple(spot)].set(top_value)


def setup_inputs(seed: int = 0) -> dict:
    arg_keys = jax.random.split(jax.random.key(seed), 7)
    return {
        "offsets": draw_offsets(jax.random.fold_in(arg_keys[6], 71), 0),
        "type_ids": touch_ends(jax.random.randint(arg_keys[1], (NCX, NCY, NCZ, ATOMS), 0, TYPES), jax.random.fold_in(arg_keys[1], 1), 0, TYPES - 1).astype(jnp.int32),
        "neighbours": draw_neighbours(jax.random.fold_in(arg_keys[6], 71), 0),
        "type_chi": jnp.clip(jax.random.uniform(arg_keys[3], (TYPES,), jnp.float32, 3.0, 7.0), 3.0, 7.0),
        "type_eta": jnp.clip(jax.random.uniform(arg_keys[4], (TYPES,), jnp.float32, 6.0, 12.0), 6.0, 12.0),
        "type_gamma": jnp.clip(jax.random.uniform(arg_keys[5], (TYPES,), jnp.float32, 0.5, 1.0), 0.5, 1.0),
    }


CELL_EDGE = 11.0
CUTOFF = 10.0
COULOMB = 14.4

def taper_value(distance):
    scaled = distance / CUTOFF
    squared = scaled * scaled
    return 1.0 + squared * squared * (-35.0 + scaled * (84.0 + scaled * (-70.0 + scaled * 20.0)))

def couplings(own_pos, own_shield, near_pos, near_shield, shifts, listed, itself):
    displace = near_pos[:, :, None, :] + shifts[:, :, None, None] - own_pos[:, None, :, None]
    dist_sq = lax.optimization_barrier(jnp.sum(displace * displace, axis=0))
    distance = jnp.sqrt(dist_sq)
    screen = own_shield[None, :, None] * near_shield[:, None, :]
    kernel = COULOMB * taper_value(distance) / jnp.cbrt(dist_sq * distance + screen)
    diagonal_mask = jnp.eye(own_pos.shape[1], dtype=bool)
    retained = listed[:, None, None] & (distance < CUTOFF) & jnp.logical_not(itself[:, None, None] & diagonal_mask[None])
    return jnp.where(retained, kernel, jnp.zeros_like(kernel))

def table_lookup(type_ids, table):
    result = jnp.zeros(type_ids.shape, table.dtype)
    for kind_index in range(table.shape[0]):
        result = jnp.where(type_ids == kind_index, table[kind_index], result)
    return result

def decode_cells(entries, local_one, local_two, local_three, width_two, width_three):
    plane_cells = (width_two + 2) * (width_three + 2)
    step_one = entries // plane_cells - 1 - local_one[..., None]
    step_two = entries // (width_three + 2) % (width_two + 2) - 1 - local_two[..., None]
    step_three = entries % (width_three + 2) - 1 - local_three[..., None]
    return (step_one, step_two, step_three)

def reference(offsets, type_ids, neighbours, type_chi, type_eta, type_gamma):
    tiles = NCX * NCY * NCZ
    sentinel = (CX + 2) * (CY + 2) * (CZ + 2)
    shape_grid = (NCX, NCY, NCZ)
    grid_one = jnp.broadcast_to(jnp.arange(NCX, dtype=jnp.int32)[:, None, None], shape_grid)
    grid_two = jnp.broadcast_to(jnp.arange(NCY, dtype=jnp.int32)[None, :, None], shape_grid)
    grid_three = jnp.broadcast_to(jnp.arange(NCZ, dtype=jnp.int32)[None, None, :], shape_grid)
    step_one, step_two, step_three = decode_cells(neighbours, grid_one % CX, grid_two % CY, grid_three % CZ, CY, CZ)
    listed = neighbours != sentinel
    itself = (step_one == 0) & (step_two == 0) & (step_three == 0)
    target = ((grid_one[..., None] + step_one) % NCX * NCY + (grid_two[..., None] + step_two) % NCY) * NCZ + (grid_three[..., None] + step_three) % NCZ
    target = jnp.where(listed, target, tiles).astype(jnp.int32).reshape(tiles, NB)
    shifts = jnp.stack([step_one, step_two, step_three], axis=-2).reshape(tiles, 3, NB).astype(jnp.float32) * CELL_EDGE
    listed = listed.reshape(tiles, NB)
    itself = itself.reshape(tiles, NB)
    chi_atom = table_lookup(type_ids, type_chi).reshape(tiles, ATOMS)
    eta_atom = table_lookup(type_ids, type_eta).reshape(tiles, ATOMS)
    shield = table_lookup(type_ids, type_gamma ** (-1.5)).reshape(tiles, ATOMS)
    positions = offsets.reshape(3, tiles, ATOMS)
    pos_all = jnp.concatenate([positions, jnp.zeros((3, 1, ATOMS), positions.dtype)], 1)
    shield_all = jnp.concatenate([shield, jnp.zeros((1, ATOMS), shield.dtype)], 0)
    own_pos = jnp.moveaxis(positions, 1, 0)
    batch_size = 16
    rounds = tiles // batch_size

    def grouped(stacked):
        return stacked.reshape((rounds, batch_size) + stacked.shape[1:])
    inputs = (grouped(own_pos), grouped(shield), grouped(target), grouped(shifts), grouped(listed), grouped(itself))
    build_batch = jax.vmap(couplings)

    def tile_pass(vectors):
        padded = jnp.concatenate([vectors, jnp.zeros((2, 1, ATOMS), vectors.dtype)], 1)

        def one_round(tile_item):
            own_block, own_screen, row_index, shifted, valid_slot, selfish = tile_item
            near_block = jnp.moveaxis(pos_all[:, row_index], 0, 1)
            near_screen = shield_all[row_index]
            blocks = build_batch(own_block, own_screen, near_block, near_screen, shifted, valid_slot, selfish)
            values = padded[:, row_index]
            return jnp.einsum('bsij,cbsj->cbi', blocks, values, precision=lax.Precision.HIGHEST)
        products = lax.map(one_round, inputs)
        return jnp.moveaxis(products, 1, 0).reshape(2, tiles, ATOMS)
    source = jnp.stack([-chi_atom, -jnp.ones_like(chi_atom)])
    diagonal = eta_atom
    solution = jnp.zeros_like(source)
    residual = source
    direction = source
    norm_now = lax.optimization_barrier(jnp.sum(residual * residual, axis=(1, 2)))
    for iteration in range(ITERS):
        coupled = tile_pass(direction)
        image_now = diagonal[None] * direction + coupled
        step_size = norm_now / lax.optimization_barrier(jnp.sum(direction * image_now, axis=(1, 2)))
        solution = solution + step_size[:, None, None] * direction
        residual = residual - step_size[:, None, None] * image_now
        norm_next = lax.optimization_barrier(jnp.sum(residual * residual, axis=(1, 2)))
        direction = residual + (norm_next / norm_now)[:, None, None] * direction
        norm_now = norm_next
    level_ratio = jnp.sum(solution[0]) / jnp.sum(solution[1])
    charges = (1000.0 * (solution[0] - level_ratio * solution[1])).reshape(NCX, NCY, NCZ, ATOMS)
    return (charges, residual.reshape(2, NCX, NCY, NCZ, ATOMS))
```

```python
import itertools

import jax
import jax.numpy as jnp
from jax import lax
from jax.experimental import pallas as pl
from jax.experimental.pallas import tpu as pltpu
from jax.sharding import PartitionSpec as P

ITERS = 3
CELL_EDGE = 11.0
CUTOFF = 10.0
COULOMB = 14.4
AXES = ("gx", "gy", "gz")
FAR = 1000.0
MESH = pl.DeviceIdType.MESH
STEPS = [d for d in itertools.product((-1, 0, 1), repeat=3)]
REMOTE = [d for d in STEPS if d != (0, 0, 0)]


def rounded_sides(step, cells):
    source, target = [], []
    for d, c in zip(step, cells):
        if d == 0:
            source.append(pl.ds(1, c))
            target.append(pl.ds(1, c))
        elif d > 0:
            source.append(pl.ds(c, 1))
            target.append(pl.ds(0, 1))
        else:
            source.append(pl.ds(1, 1))
            target.append(pl.ds(c + 1, 1))
    return tuple(source), tuple(target)


def make_kernel(sizes, groups, cells, atoms, types, rows):
    width = tuple(c + 2 for c in cells)
    tiles = cells[0] * cells[1] * cells[2]
    local = list(itertools.product(*[range(c) for c in cells]))
    padded = list(itertools.product(*[range(w) for w in width]))
    own = tuple(slice(1, 1 + c) for c in cells)
    group_sizes = []
    for axes in groups:
        count = 1
        for a in axes:
            count = count * sizes[a]
        group_sizes.append(count)

    def linear(place):
        return (place[0] * width[1] + place[1]) * width[2] + place[2]

    def kernel(*refs):
        off_ref, type_ref, list_ref, chi_ref, eta_ref, gamma_ref, charge_ref, resid_ref = refs[:8]
        (fields, geometry, columns, far, blocks, sums, resid, along, *rest) = refs[8:]
        images = rest[:ITERS]
        rest = rest[ITERS:]
        parts = rest[: len(groups)]
        halo_send, halo_recv, sum_send, sum_recv = rest[len(groups) :]

        me = {a: lax.axis_index(a) for a in AXES}

        def neighbour(step):
            return tuple(
                lax.rem(me[a] + (d + sizes[a]), sizes[a]) for a, d in zip(AXES, step)
            )

        def member(axes, hop):
            rank = 0
            count = 1
            for a in axes:
                rank = rank * sizes[a] + me[a]
                count = count * sizes[a]
            rank = lax.rem(rank + hop, count)
            place = dict(me)
            for a in reversed(axes):
                place[a] = lax.rem(rank, sizes[a])
                rank = rank // sizes[a]
            return tuple(place[a] for a in AXES)

        def lookup(kinds, table):
            result = jnp.zeros(kinds.shape, jnp.float32)
            for k in range(types):
                result = jnp.where(kinds == float(k), table[k], result)
            return result

        for x, y, z in local:
            for f in range(3):
                fields[x + 1, y + 1, z + 1, f : f + 1, :] = off_ref[f, x, y, z : z + 1, :]
            fields[x + 1, y + 1, z + 1, 3:4, :] = type_ref[x, y, z : z + 1, :].astype(jnp.float32)

        barrier = pltpu.get_barrier_semaphore()
        greeted = 0
        for axes, count in zip(groups, group_sizes):
            for hop in range(1, count):
                pl.semaphore_signal(
                    barrier, inc=1, device_id=member(axes, hop), device_id_type=MESH
                )
                greeted += 1
        if len(groups) > 1:
            for step in REMOTE:
                pl.semaphore_signal(
                    barrier, inc=1, device_id=neighbour(step), device_id_type=MESH
                )
                greeted += 1
        pl.semaphore_wait(barrier, greeted)

        def halo(buffer, stage):
            copies = []
            for n, step in enumerate(REMOTE):
                source, target = rounded_sides(step, cells)
                copies.append(
                    pltpu.make_async_remote_copy(
                        src_ref=buffer.at[source],
                        dst_ref=buffer.at[target],
                        send_sem=halo_send.at[n],
                        recv_sem=halo_recv.at[stage, n],
                        device_id=neighbour(step),
                        device_id_type=MESH,
                    )
                )
            for copy in copies:
                copy.start()
            return copies

        def finish(copies):
            for copy in copies:
                copy.wait_recv()
            for copy in copies:
                copy.wait_send()

        moving = halo(fields, 0)

        def tenth(values, f, place):
            return (values + CELL_EDGE * (place[f] - 1.0)) * (1.0 / CUTOFF)

        def sigma(kinds):
            root = lax.rsqrt(lookup(kinds, gamma_ref))
            return root * root * root * (CUTOFF**-1.5)

        for t, (x, y, z) in enumerate(local):
            place = (x + 1, y + 1, z + 1)
            for f in range(4):
                row = fields[x + 1, y + 1, z + 1, f : f + 1, :]
                row = tenth(row, f, place) if f < 3 else sigma(row)
                columns[t, f] = jnp.transpose(jnp.broadcast_to(row, (atoms, atoms)))
        entries = jnp.concatenate(
            [list_ref[x, y, z : z + 1, :] - linear((x + 1, y + 1, z + 1)) for x, y, z in local], 0
        )
        for n, step in enumerate(STEPS):
            found = jnp.max(
                jnp.where(entries == linear(step), 1.0, 0.0), axis=1, keepdims=True
            )
            far[n] = jnp.broadcast_to((1.0 - found) * FAR, (tiles, atoms))

        finish(moving)

        for x, y, z in padded:
            place = (x, y, z)
            kinds = fields[x, y, z, 3:4, :]
            for f in range(3):
                geometry[x, y, z, f : f + 1, :] = tenth(fields[x, y, z, f : f + 1, :], f, place)
            geometry[x, y, z, 3:4, :] = sigma(kinds)
            resid[x, y, z, 0:1, :] = -lookup(kinds, chi_ref)
            resid[x, y, z, 1:2, :] = jnp.full((1, atoms), -1.0, jnp.float32)

        slabs = atoms // rows

        def spot(index):
            t = index // slabs
            at = pl.multiple_of((index % slabs) * rows, rows)
            z = t % cells[2]
            y = (t // cells[2]) % cells[1]
            x = t // (cells[2] * cells[1])
            return t, at, (x + 1, y + 1, z + 1)

        def build(index, carry):
            t, at, (x, y, z) = spot(index)
            own_part = [columns[t, f, pl.ds(at, rows), :] for f in range(4)]
            total_s = jnp.zeros((rows, atoms), jnp.float32)
            total_t = jnp.zeros((rows, atoms), jnp.float32)
            for n, (a, b, c) in enumerate(STEPS):
                near = [geometry[x + a, y + b, z + c, f : f + 1, :] for f in range(4)]
                near[0] = near[0] + far[n, pl.ds(t, 1), :]
                dx = near[0] - own_part[0]
                dy = near[1] - own_part[1]
                dz = near[2] - own_part[2]
                square = dx * dx + dy * dy + dz * dz
                if (a, b, c) == (0, 0, 0):
                    i = lax.broadcasted_iota(jnp.int32, (rows, atoms), 0) + at
                    j = lax.broadcasted_iota(jnp.int32, (rows, atoms), 1)
                    square = jnp.where(i == j, 4.0, square)
                u = square * lax.rsqrt(square)
                w = jnp.maximum(1.0 - u, 0.0)
                w = w * w
                w = w * w
                shape = (u + 0.5) * (square + 0.2) - 0.05
                cube = square * u + own_part[3] * near[3]
                block = w * shape * jnp.exp2(jnp.log2(cube) * (-1.0 / 3.0))
                blocks[t, n, pl.ds(at, rows), :] = block
                total_s = total_s + block * resid[x + a, y + b, z + c, 0:1, :]
                total_t = total_t - block
            sums[t, 0, pl.ds(at, rows), :] = total_s
            sums[t, 1, pl.ds(at, rows), :] = total_t
            return carry

        def again(index, carry):
            t, at, (x, y, z) = spot(index)
            total_s = jnp.zeros((rows, atoms), jnp.float32)
            total_t = jnp.zeros((rows, atoms), jnp.float32)
            for n, (a, b, c) in enumerate(STEPS):
                block = blocks[t, n, pl.ds(at, rows), :]
                total_s = total_s + block * resid[x + a, y + b, z + c, 0:1, :]
                total_t = total_t + block * resid[x + a, y + b, z + c, 1:2, :]
            sums[t, 0, pl.ds(at, rows), :] = total_s
            sums[t, 1, pl.ds(at, rows), :] = total_t
            return carry

        scale = 20.0 * COULOMB / CUTOFF
        ones = jnp.ones((8, atoms), jnp.float32)
        eta = [lookup(fields[x + 1, y + 1, z + 1, 3:4, :], eta_ref) for x, y, z in local]

        def collect(image):
            for t, (x, y, z) in enumerate(local):
                for s in range(2):
                    row = lax.dot_general(
                        ones,
                        sums[t, s],
                        (((1,), (1,)), ((), ())),
                        precision=lax.Precision.HIGHEST,
                        preferred_element_type=jnp.float32,
                    )[0:1]
                    here = resid[x + 1, y + 1, z + 1, s : s + 1, :]
                    image[x + 1, y + 1, z + 1, s : s + 1, :] = eta[t] * here + scale * row

        lane = lax.broadcasted_iota(jnp.int32, (2, atoms), 1)

        def over_own(values):
            return jnp.sum(jnp.sum(values, axis=(0, 1, 2)), axis=1, keepdims=True)

        def packed(values):
            message = jnp.zeros((2, atoms), jnp.float32)
            for k, value in enumerate(values):
                message = jnp.where(lane == k, value, message)
            return message

        def start_sum(g, stage):
            axes, count = groups[g], group_sizes[g]
            start = sum(group_sizes[:g]) - g
            copies = []
            for hop in range(1, count):
                copies.append(
                    pltpu.make_async_remote_copy(
                        src_ref=parts[g].at[stage, 0],
                        dst_ref=parts[g].at[stage, hop],
                        send_sem=sum_send.at[start + hop - 1],
                        recv_sem=sum_recv.at[stage, start + hop - 1],
                        device_id=member(axes, hop),
                        device_id_type=MESH,
                    )
                )
            for copy in copies:
                copy.start()
            return copies

        def exchange(values, image, stage):
            parts[0][stage, 0] = packed(values)
            moving = halo(image, stage + 1) if stage + 1 < ITERS else []
            copies = start_sum(0, stage)
            for g in range(len(groups)):
                finish(copies)
                total = jnp.sum(parts[g][stage], axis=0)
                if g + 1 < len(groups):
                    parts[g + 1][stage, 0] = total
                    copies = start_sum(g + 1, stage)
            finish(moving)
            return [
                jnp.sum(jnp.where(lane == k, total, 0.0), axis=1, keepdims=True)
                for k in range(len(values))
            ]

        lax.fori_loop(0, tiles * slabs, build, 0)
        collect(images[0])
        direction = resid[own]
        norm_now, curvature = exchange(
            [over_own(direction * direction), over_own(direction * images[0][own])], images[0], 0
        )
        step_size = norm_now / curvature
        answer = jnp.zeros_like(direction)
        sum_answer = jnp.zeros_like(norm_now)
        along[...] = images[0][...]
        carried = (norm_now, norm_now, norm_now, jnp.zeros_like(norm_now))
        for iteration in range(ITERS):
            answer = answer + step_size * direction
            if iteration + 1 == ITERS:
                last = resid[own] - step_size * along[own]
                break
            resid[...] = resid[...] - step_size * along[...]
            lax.fori_loop(0, tiles * slabs, again, 0)
            image = images[iteration + 1]
            collect(image)
            here = resid[own]
            values = [over_own(here * here), over_own(here * image[own])]
            ends = iteration + 2 == ITERS
            if ends:
                values = values + [over_own(answer), over_own(here), over_own(direction)]
            norm_next, curvature, *others = exchange(values, image, iteration + 1)
            growth = norm_next / norm_now
            step_size = norm_next / (curvature - growth * norm_next / step_size)
            direction = here + growth * direction
            if ends:
                along[own] = image[own] + growth * along[own]
                totals = others[0] + step_size * (others[1] + growth * others[2])
            else:
                along[...] = image[...] + growth * along[...]
            norm_now = norm_next

        level = totals[0:1] / totals[1:2]
        for t, (x, y, z) in enumerate(local):
            charge_ref[x, y, z : z + 1, :] = 1000.0 * (
                answer[x, y, z, 0:1] - level * answer[x, y, z, 1:2]
            )
            for s in range(2):
                resid_ref[s, x, y, z : z + 1, :] = last[x, y, z, s : s + 1]

    scratch = [
        pltpu.VMEM(width + (4, atoms), jnp.float32),
        pltpu.VMEM(width + (4, atoms), jnp.float32),
        pltpu.VMEM((tiles, 4, atoms, atoms), jnp.float32),
        pltpu.VMEM((len(STEPS), tiles, atoms), jnp.float32),
        pltpu.VMEM((tiles, len(STEPS), atoms, atoms), jnp.float32),
        pltpu.VMEM((tiles, 2, atoms, atoms), jnp.float32),
        pltpu.VMEM(width + (2, atoms), jnp.float32),
        pltpu.VMEM(width + (2, atoms), jnp.float32),
    ]
    scratch += [pltpu.VMEM(width + (2, atoms), jnp.float32) for _ in range(ITERS)]
    scratch += [pltpu.VMEM((ITERS, count, 2, atoms), jnp.float32) for count in group_sizes]
    hops = sum(group_sizes) - len(groups)
    scratch += [
        pltpu.SemaphoreType.DMA((len(REMOTE),)),
        pltpu.SemaphoreType.DMA((ITERS, len(REMOTE))),
        pltpu.SemaphoreType.DMA((hops,)),
        pltpu.SemaphoreType.DMA((ITERS, hops)),
    ]
    return kernel, scratch


def solution(mesh):
    sizes = {a: mesh.shape[a] for a in AXES}
    devices = sizes["gx"] * sizes["gy"] * sizes["gz"]
    groups = (AXES,) if devices <= 64 else tuple((a,) for a in AXES)

    def per_device(offsets, type_ids, neighbours, type_chi, type_eta, type_gamma):
        cells = offsets.shape[1:4]
        atoms = offsets.shape[4]
        types = type_chi.shape[0]
        kernel, scratch = make_kernel(sizes, groups, cells, atoms, types, 32)
        vmem = pl.BlockSpec(memory_space=pltpu.VMEM)
        smem = pl.BlockSpec(memory_space=pltpu.SMEM)
        return pl.pallas_call(
            kernel,
            out_shape=(
                jax.ShapeDtypeStruct(cells + (atoms,), jnp.float32),
                jax.ShapeDtypeStruct((2,) + cells + (atoms,), jnp.float32),
            ),
            in_specs=[vmem, vmem, vmem, smem, smem, smem],
            out_specs=(vmem, vmem),
            scratch_shapes=scratch,
            compiler_params=pltpu.CompilerParams(
                collective_id=0, has_side_effects=True, vmem_limit_bytes=48 * 1024 * 1024
            ),
        )(offsets, type_ids, neighbours, type_chi, type_eta, type_gamma)

    placed = (
        P(None, "gx", "gy", "gz", None),
        P("gx", "gy", "gz", None),
        P("gx", "gy", "gz", None),
        P(),
        P(),
        P(),
    )
    return jax.shard_map(
        per_device,
        mesh=mesh,
        in_specs=placed,
        out_specs=(P("gx", "gy", "gz", None), P(None, "gx", "gy", "gz", None)),
        check_vma=False,
    )
```
